256 devices in a mesh: grp: 4 (over x, y), space: 64 (over z, core).
Axes of the slice: x: 2, y: 2, z: 32, core: 2. Of those that a mesh axis runs over, the one named last changes fastest.
The devices are a block of a 4x8x32 slice.
Arguments:
- propagator: bfloat16 [8, 3, 4, 12, 131072], P('grp', None, None, None, 'space'), parts along dimension 0, may hold values from -6 to 6
- eigvecs: bfloat16 [8, 3, 256, 131072], P('grp', None, None, 'space'), parts along dimension 0, may hold values from -16 to 16
- operator_weights: float32 [512, 2, 256], P('grp'), parts along dimension 0, may hold values from -0.375 to 0.375
- sink_time: int32 [4], P('grp'), parts along dimension 0, may hold values from 0 to 127
- term_index: int32 [48, 3], replicated, may hold values from 0 to 11
- term_sign: int32 [48], replicated, may hold values from 0 to 1
- solver_order: int32 [131072], P('space'), may hold values from 0 to 131071, as said below
Outputs:
- solver_source: bfloat16 [8, 3, 4, 12, 131072], P('grp', None, None, None, 'space'), parts along dimension 0
The draws below stay inside these ranges and needn't reach their ends.
There are 4 independent parts, one for each index of `grp`. The reference program is written for one: setup_inputs(seed, part) draws one part's arguments, and reference() takes and returns one part's arrays. A program takes and returns all parts, laid end to end along the dimension named above; an argument that names none is the same for every part. Nothing has to cross between parts.
Inputs may be any that keep to these rules, and one draw needn't show every extreme that they name: solver_order is a permutation of the sites; split into blocks of 2048 positions and each block into pieces of 32, piece d of block e holds only sites d * 2048 to (d + 1) * 2048 - 1.
All inputs are finite; a program needn't handle non-finite values.
Results may differ from the reference program's by a relative error of at most 0.006.
Values may be sent and summed in bfloat16 or wider, within the bound.
A program may use at most 64 MiB of HBM per device.

```python
import math
import jax
import jax.numpy as jnp
from jax import lax

NVEC = 256
NMOM = 4
NTERM = 48
EXTENT = 64
TIME_EXTENT = 128
SITES_DEV = 2048
SITES = 131072
PAIR = 32


def one_permutation(block_key):
    return jax.random.permutation(block_key, SITES_DEV)


def draw_solver_order(key, part):
    owners_count = SITES // SITES_DEV
    block_keys = jax.random.split(jax.random.fold_in(key, 17), owners_count)
    shuffled = jax.vmap(one_permutation)(block_keys).astype(jnp.int32).reshape(owners_count, owners_count, PAIR)
    owner_start = (jnp.arange(owners_count, dtype=jnp.int32) * SITES_DEV)[:, None, None]
    ordered = (shuffled + owner_start).transpose(1, 0, 2)
    return ordered.reshape(SITES)


def place_ends(values, stream_key, smallest, top_value):
    spot = [jax.random.randint(jax.random.fold_in(stream_key, axis), (), 0, length) for axis, length in enumerate(values.shape)]
    main_axis = values.shape.index(max(values.shape))
    next_to = spot[:main_axis] + [(spot[main_axis] + 1) % values.shape[main_axis]] + spot[main_axis + 1:]
    return values.at[tuple(spot)].set(smallest).at[tuple(next_to)].set(top_value)


def spiked(entries, own_key, source, target, blocks, factor):
    def block_of(dim):
        return (jnp.arange(entries.shape[dim]) // (entries.shape[dim] // blocks)).reshape((-1,) + (1,) * (entries.ndim - 1 - dim))

    near = jax.random.permutation(own_key, blocks)[block_of(target)]
    far = (block_of(target) + blocks // 2) % blocks
    return jnp.where((block_of(source) == near) | (block_of(source) == far), factor * entries, entries)


def steps_of(rng, extent, shards, smallest, top_value):
    loudness = 1.0
    for position, parts in shards:
        draws = jax.random.uniform(jax.random.fold_in(jax.random.fold_in(rng, 6), position), (parts,), jnp.float32, smallest / len(shards), top_value / len(shards))
        loudness = loudness * jnp.repeat(jnp.exp(draws), extent[position] // parts).reshape((-1,) + (1,) * (len(extent) - 1 - position))
    return loudness


def normal_values(own_key, dims, scale, bound, cuts=(), kind=jnp.bfloat16):
    result = jax.random.normal(own_key, dims, jnp.float32) * scale
    if len(cuts) > 0:
        result = steps_of(own_key, dims, cuts, -0.22, 0.18) * result
    return jnp.clip(result, min=-bound, max=bound).astype(kind)


def gaussian_with(key, dims, spread, limit, cuts, heavy, held_as=jnp.bfloat16):
    values = spread * jax.random.normal(key, dims, jnp.float32)
    if cuts:
        values = values * steps_of(key, dims, cuts, -0.22, 0.18)
    return jnp.clip(spiked(values, jax.random.fold_in(key, 3), *heavy), -limit, limit).astype(held_as)


def setup_inputs(seed: int = 0, part: int = 0) -> dict:
    splits = jax.random.split(jax.random.key(seed), 8)
    part_splits = jax.random.split(jax.random.fold_in(splits[7], part), 8)
    return {
        "propagator": normal_values(part_splits[0], (2, 3, 4, 12, SITES), 1.0, 6.0, ((4, 64),)),
        "eigvecs": gaussian_with(part_splits[1], (2, 3, NVEC, SITES), 1.0, 16.0, ((3, 64),), (3, 2, 64, 4.0)),
        "operator_weights": normal_values(part_splits[2], (TIME_EXTENT, 2, NVEC), NVEC ** -0.5, 0.375, (), jnp.float32),
        "sink_time": jax.random.randint(part_splits[3], (1,), 0, TIME_EXTENT).astype(jnp.int32),
        "term_index": place_ends(jax.random.randint(splits[4], (NTERM, 3), 0, 12), jax.random.fold_in(splits[4], 1), 0, 11).astype(jnp.int32),
        "term_sign": place_ends(jax.random.randint(splits[5], (NTERM,), 0, 2), jax.random.fold_in(splits[5], 1), 0, 1).astype(jnp.int32),
        "solver_order": draw_solver_order(jax.random.fold_in(splits[7], 71), part),
    }


MOMENTA = ((0, 0, 0), (1, 0, 0), (0, 1, 0), (0, 0, 1))
PRECISE = lax.Precision.HIGHEST

def phase_tables(offset, length):
    site_index = offset + jnp.arange(length, dtype=jnp.int32)
    coord_x = site_index % EXTENT
    coord_y = site_index // EXTENT % EXTENT
    coord_z = site_index // (EXTENT * EXTENT)
    windings = jnp.stack([(step_x * coord_x + step_y * coord_y + step_z * coord_z) % EXTENT for step_x, step_y, step_z in MOMENTA])
    angles = windings.astype(jnp.float32) * (2.0 * math.pi / EXTENT)
    return (jnp.cos(angles), jnp.sin(angles))

def phased_rows(prop_colour, cosine_table, sine_table):
    real_part = prop_colour[0].astype(jnp.float32)[None]
    imag_part = prop_colour[1].astype(jnp.float32)[None]
    cos_rows = cosine_table[:, None, None, :]
    sin_rows = sine_table[:, None, None, :]
    turned = jnp.stack([cos_rows * real_part + sin_rows * imag_part, cos_rows * imag_part - sin_rows * real_part])
    return turned.astype(jnp.bfloat16).reshape(-1, turned.shape[-1])

def project(eig_colour, phased, scale_in):
    from_real = jnp.dot(eig_colour[0], phased.T, preferred_element_type=jnp.float32).reshape(-1, 2, NMOM, 48)
    from_imag = jnp.dot(eig_colour[1], phased.T, preferred_element_type=jnp.float32).reshape(-1, 2, NMOM, 48)
    real_part = from_real[:, 0] + from_imag[:, 1]
    imag_part = from_real[:, 1] - from_imag[:, 0]
    return jnp.stack([real_part, imag_part]) * scale_in

def assemble(pieces):
    stacked = jnp.stack(pieces)
    vectors = stacked.shape[2]
    return stacked.transpose(3, 1, 2, 0, 4).reshape(NMOM, 2, vectors, 144)

def weighted_total(blocks, weights):
    real_sum = jnp.einsum('k,pkc->pc', weights[0], blocks[:, 0], precision=PRECISE) - jnp.einsum('k,pkc->pc', weights[1], blocks[:, 1], precision=PRECISE)
    imag_sum = jnp.einsum('k,pkc->pc', weights[0], blocks[:, 1], precision=PRECISE) + jnp.einsum('k,pkc->pc', weights[1], blocks[:, 0], precision=PRECISE)
    return jnp.stack([real_sum, imag_sum], axis=1)

def term_tables(term_index, term_sign):
    channels = jnp.arange(12, dtype=jnp.int32)
    first_pick = (term_index[:, 0:1] == channels[None]).astype(jnp.float32)
    second_pick = (term_index[:, 1:2] == channels[None]).astype(jnp.float32)
    sign_values = (2 * term_sign - 1).astype(jnp.float32)
    placement = (term_index[None, :, 2] == channels[:, None]).astype(jnp.float32) * sign_values[None]
    return (first_pick, second_pick, placement)

def contract(blocks, weighted, first_pick, second_pick, placement):
    vectors = blocks.shape[2]
    block_grid = blocks.reshape(NMOM, 2, vectors, 12, 12)
    first_terms = jnp.einsum('mi,pqkij->pqkmj', first_pick, block_grid, precision=PRECISE)
    second_terms = jnp.einsum('mi,pqij->pqmj', second_pick, weighted.reshape(NMOM, 2, 12, 12), precision=PRECISE)[:, :, None]
    real_part = first_terms[:, 0] * second_terms[:, 0] - first_terms[:, 1] * second_terms[:, 1]
    imag_part = first_terms[:, 0] * second_terms[:, 1] + first_terms[:, 1] * second_terms[:, 0]
    product = jnp.stack([real_part, imag_part], axis=1)
    return jnp.einsum('cm,pqkmj->pqkcj', placement, product, precision=PRECISE).reshape(NMOM, 2, vectors, 144)

def rebuild(coeffs, eig_colour, colour, cosine_table, sine_table, scale_out):
    vectors = coeffs.shape[2]
    colour_block = coeffs.reshape(NMOM, 2, vectors, 3, 48)[:, :, :, colour]
    coeff_table = colour_block.transpose(2, 1, 0, 3).reshape(vectors, 2 * NMOM * 48)
    from_real = jnp.dot(coeff_table.T, eig_colour[0], preferred_element_type=jnp.float32).reshape(2, NMOM, 48, -1)
    from_imag = jnp.dot(coeff_table.T, eig_colour[1], preferred_element_type=jnp.float32).reshape(2, NMOM, 48, -1)
    real_part = from_real[0] - from_imag[1]
    imag_part = from_real[1] + from_imag[0]
    cos_rows = cosine_table[:, None, :]
    sin_rows = sine_table[:, None, :]
    out_real = lax.optimization_barrier(jnp.sum(cos_rows * real_part - sin_rows * imag_part, axis=0))
    out_imag = lax.optimization_barrier(jnp.sum(cos_rows * imag_part + sin_rows * real_part, axis=0))
    return jnp.stack([out_real, out_imag]) * scale_out

def reference(propagator, eigvecs, operator_weights, sink_time, term_index, term_sign, solver_order):
    cosine_table, sine_table = phase_tables(0, SITES)
    scale_in = 1.0 / math.sqrt(3.0 * SITES)
    pieces = []
    for colour in range(3):
        phased = phased_rows(propagator[:, colour], cosine_table, sine_table)
        pieces.append(project(eigvecs[:, colour], phased, scale_in))
    blocks = assemble(pieces)
    weights = lax.dynamic_index_in_dim(operator_weights, sink_time[0], 0, keepdims=False)
    first_pick, second_pick, placement = term_tables(term_index, term_sign)
    weighted = weighted_total(blocks, weights)
    coeffs = contract(blocks, weighted, first_pick, second_pick, placement).astype(jnp.bfloat16)
    scale_out = 1.0 / math.sqrt(NMOM * NVEC)
    colours = [rebuild(coeffs, eigvecs[:, colour], colour, cosine_table, sine_table, scale_out) for colour in range(3)]
    source = jnp.stack(colours, axis=1).astype(jnp.bfloat16).reshape(2, 3, 4, 12, SITES)
    return jnp.take(source, solver_order, axis=4)
```

```python
import functools
import math

import jax
import jax.numpy as jnp
import ml_dtypes
import numpy as np
from jax import lax
from jax.experimental import pallas as pl
from jax.experimental.pallas import tpu as pltpu
from jax.sharding import Mesh
from jax.sharding import PartitionSpec as P

NVEC = 256
NMOM = 4
NTERM = 48
EXTENT = 64
SPACE = ("space_0", "space_1")
MESH = pl.DeviceIdType.MESH
PRECISE = lax.Precision.HIGHEST
F32 = jnp.float32
BF16 = jnp.bfloat16

LANES = 128
HALF = 24
CHUNK = 512
GROUP = 256


def fixed_tables(length, chips):
    assert 2 * length == EXTENT * EXTENT
    site = np.arange(length)
    turn = 2.0 * np.pi / EXTENT
    angle_x = turn * (site % EXTENT)
    tables, pieces = [], []
    for core in range(2):
        angle_y = turn * ((core * length + site) // EXTENT % EXTENT)
        rows = np.stack([np.cos(angle_x), np.sin(angle_x), np.cos(angle_y), np.sin(angle_y)]).astype(np.float32)
        tables.append(np.concatenate([rows, np.zeros_like(rows)]))
        high = rows.astype(ml_dtypes.bfloat16)
        middle = (rows - high.astype(np.float32)).astype(ml_dtypes.bfloat16)
        low = (rows - high.astype(np.float32) - middle.astype(np.float32)).astype(ml_dtypes.bfloat16)
        pieces.append(np.concatenate([high, middle, low, np.zeros_like(high)]))
    angle_z = turn * (np.arange(chips) % EXTENT)
    chip_phase = np.zeros((chips, 8, LANES), np.float32)
    chip_phase[:, 0] = np.cos(angle_z)[:, None]
    chip_phase[:, 1] = np.sin(angle_z)[:, None]
    pick = np.zeros((2, 8, 512), np.float32)
    fold = np.zeros((2, 512, LANES), np.float32)
    for colour in range(3):
        for row in range(6):
            for u in range(HALF):
                lane = colour * 144 + row * HALF + u
                pick[0, row, lane] = 1.0
                pick[1, row ^ 1, lane] = 1.0 if row % 2 == 0 else -1.0
                fold[0, lane, colour * HALF + u] = 1.0
                fold[1, lane, 48 + colour * HALF + u] = 1.0
    return np.stack(tables), np.stack(pieces), chip_phase, pick, fold


def term_matrices(term_index, term_sign):
    row = jnp.arange(LANES, dtype=jnp.int32)[:, None]
    lane = jnp.arange(384, dtype=jnp.int32)[None]
    spread = jnp.pad(jnp.repeat(term_index.T, 6, axis=1), ((0, 0), (0, 384 - 288)), constant_values=-1)
    signs = jnp.pad(jnp.repeat((2 * term_sign - 1).astype(F32), 6), (0, 384 - 288))
    same = (row % 6 == lane % 6) & (row < 72)
    first = jnp.where(same & (row // 6 == spread[0][None]), 1.0, 0.0)
    second = jnp.where(same & (row // 6 == spread[1][None]), 1.0, 0.0)
    place = jnp.where(same & (row // 6 == spread[2][None]), signs[None], 0.0)
    return jnp.stack([first, second, place]).astype(F32)


def dot(a, b, precision=None):
    return lax.dot_general(a, b, (((1,), (0,)), ((), ())), preferred_element_type=F32, precision=precision)


def dot_nt(a, b, precision=None):
    return lax.dot_general(a, b, (((1,), (1,)), ((), ())), preferred_element_type=F32, precision=precision)


def far_first(step, count):
    half = (step + 1) // 2
    return count // 2 + half * (1 - 2 * (step % 2))


def swap_blocks(tiles, lane_block):
    result = []
    for g in range(4):
        message = tiles[0] if g == 0 else pltpu.roll(tiles[0], (-g * 32) % LANES, 1)
        for q in range(1, 4):
            moved = tiles[q] if q == g else pltpu.roll(tiles[q], ((q - g) * 32) % LANES, 1)
            message = jnp.where(lane_block == q, moved, message)
        result.append(message)
    return result


def lane_blocks():
    return lax.broadcasted_iota(jnp.int32, (72, LANES), 1) // 32


def whole_kernel(
    chips, length, scale_in, scale_out,
    eig, prop, idx_rows, weights, tables, pieces, chip_phase, pick, fold, terms,
    out,
    eig_v, prop_v, accs, full, from_core, chip_sum, rs_send, rs_recv, idx_recv,
    perm, eig_p, phase_p, gathered, coeff_t, left, source, to_send,
    load_sem, core_sem, idx_sem, rs_sem, near_sem, ag_sem, side_sem, both_sem, all_sem,
):
    z = lax.axis_index("space_0")
    core = lax.axis_index("space_1")
    devices = 2 * chips
    me = 2 * z + core
    other = 1 - core

    def device(chip, on_core):
        return {"space_0": chip, "space_1": on_core}

    def remote(src, dst, send_sem, recv_sem, chip, on_core):
        return pltpu.make_async_remote_copy(
            src_ref=src, dst_ref=dst, send_sem=send_sem, recv_sem=recv_sem,
            device_id=device(chip, on_core), device_id_type=MESH,
        )

    loads = []
    for a in range(3):
        for q in range(2):
            loads.append(pltpu.make_async_copy(prop.at[q, a], prop_v.at[q, a], load_sem.at[4 * a + q]))
            loads.append(pltpu.make_async_copy(eig.at[q, a], eig_v.at[a, pl.ds(q * NVEC, NVEC)], load_sem.at[4 * a + 2 + q]))
    for load in loads:
        load.start()

    barrier = pltpu.get_barrier_semaphore()

    def greet(i, carry):
        peer = lax.rem(me + i, devices)
        pl.semaphore_signal(barrier, inc=1, device_id=device(peer // 2, lax.rem(peer, 2)), device_id_type=MESH)
        return carry

    lax.fori_loop(1, devices, greet, 0)

    for a in range(3):
        for load in loads[4 * a : 4 * a + 4]:
            load.wait()
        for h in range(2):
            accs[h, a] = jnp.zeros((NVEC, 144), F32)

        def project(ci, carry, a=a):
            sites = pl.ds(pl.multiple_of(ci * CHUNK, CHUNK), CHUNK)
            table = tables[core, :, sites]
            cos_x, sin_x, cos_y, sin_y = (table[n : n + 1] for n in range(4))
            real = prop_v[0, a, :, :, sites].astype(F32)
            imag = prop_v[1, a, :, :, sites].astype(F32)
            for h in range(2):
                re = jnp.concatenate([real[s, 6 * h : 6 * h + 6] for s in range(4)], axis=0)
                im = jnp.concatenate([imag[s, 6 * h : 6 * h + 6] for s in range(4)], axis=0)
                re_x, im_x = cos_x * re + sin_x * im, cos_x * im - sin_x * re
                re_y, im_y = cos_y * re + sin_y * im, cos_y * im - sin_y * re
                with_real = jnp.concatenate([re, im, re_x, im_x, re_y, im_y], axis=0).astype(BF16)
                with_imag = jnp.concatenate([im, -re, im_x, -re_x, im_y, -re_y], axis=0).astype(BF16)
                accs[h, a] += dot_nt(eig_v[a, 0:NVEC, sites], with_real) + dot_nt(eig_v[a, NVEC : 2 * NVEC, sites], with_imag)
            return carry

        lax.fori_loop(0, length // CHUNK, project, 0)

    def join_colours(rb, carry):
        rows = pl.ds(pl.multiple_of(rb * 32, 32), 32)
        for h in range(2):
            full[h, rows] = jnp.concatenate([accs[h, a, rows] for a in range(3)] + [jnp.zeros((32, 80), F32)], axis=1)
        return carry

    lax.fori_loop(0, NVEC // 32, join_colours, 0)

    pl.semaphore_wait(barrier, devices - 1)

    to_core = remote(full.at[other], from_core, core_sem.at[0], core_sem.at[1], z, other)
    to_core.start()

    def send_index(i, carry):
        peer = lax.rem(me + far_first(i, devices), devices)
        remote(idx_rows.at[peer], idx_recv.at[me], idx_sem.at[0], idx_sem.at[1], peer // 2, lax.rem(peer, 2)).start()
        return carry

    lax.fori_loop(0, devices - 1, send_index, 0)
    idx_recv[me] = idx_rows[me]

    to_core.wait()
    chip_sum[...] = (full[core] + from_core[...]) * scale_in

    by_weight = dot(weights[...], chip_sum[...], PRECISE)
    weighted_rows = by_weight[0:1] * pick[0] + by_weight[1:2] * pick[1]
    weighted_part = dot(weighted_rows, fold[1], PRECISE)
    beside = jnp.concatenate([jnp.zeros((8, 384), F32), weighted_part], axis=1)

    def pack(zz, carry):
        rows = pl.ds(pl.multiple_of(zz * 8, 8), 8)
        rs_send[zz] = (chip_sum[rows] + beside).astype(BF16)
        return carry

    lax.fori_loop(0, chips, pack, 0)

    def send_part(i, carry):
        peer = lax.rem(z + far_first(i, chips), chips)
        remote(rs_send.at[peer], rs_recv.at[z], rs_sem.at[0], rs_sem.at[1], peer, core).start()
        return carry

    lax.fori_loop(0, chips - 1, send_part, 0)
    rs_recv[z] = rs_send[z]

    some = pl.ds(0, devices - 1)
    pltpu.make_async_copy(idx_recv.at[some], idx_recv.at[some], idx_sem.at[1]).wait()

    def reorder(g, carry):
        columns = pl.ds(pl.multiple_of(g * GROUP, GROUP), GROUP)
        wanted = jnp.concatenate(
            [sum(idx_recv[g * 8 + 4 * k + n] for n in range(4)) for k in range(2)], axis=1
        ) - me * length

        def one_hot(rb, inner):
            rows = pl.ds(pl.multiple_of(rb * 64, 64), 64)
            here = lax.broadcasted_iota(jnp.int32, (64, GROUP), 0) + rb * 64
            perm[rows] = jnp.where(here == wanted, 1.0, 0.0).astype(BF16)
            return inner

        lax.fori_loop(0, length // 64, one_hot, 0)
        for a in range(3):
            eig_p[a, :, columns] = dot(eig_v[a], perm[...]).astype(BF16)
        turned = dot(pieces[core], perm[...])
        phase_p[:, columns] = jnp.concatenate([turned[0:4] + turned[4:8] + turned[8:12], jnp.zeros((4, GROUP), F32)], axis=0)
        return carry

    lax.fori_loop(0, length // GROUP, reorder, 0)

    some = pl.ds(0, chips - 1)
    pltpu.make_async_copy(rs_recv.at[some], rs_recv.at[some], rs_sem.at[1]).wait()
    total = jnp.zeros((8, 512), F32)
    total_cos = jnp.zeros((8, 512), F32)
    total_sin = jnp.zeros((8, 512), F32)
    for zz in range(chips):
        part = rs_recv[zz].astype(F32)
        total = total + part
        total_cos = total_cos + chip_phase[zz, 0:1, 0:1] * part
        total_sin = total_sin + chip_phase[zz, 1:2, 0:1] * part
    masks = pick[0]
    blocks = [total * masks[r : r + 1] for r in range(6)]
    blocks.append(total_cos * masks[0:1] + total_sin * masks[1:2])
    blocks.append(total_cos * masks[1:2] - total_sin * masks[0:1])
    block_rows = dot(jnp.concatenate(blocks, axis=0), fold[0], PRECISE)
    tails = [pltpu.roll(t[:, 384:512], LANES - 48, 1) for t in (total, total_cos, total_sin)]
    weighted = jnp.concatenate(
        [tails[0][0:6], tails[1][0:1] + tails[2][1:2], tails[1][1:2] - tails[2][0:1]], axis=0
    )
    first = dot(block_rows, terms[0], PRECISE)
    second = dot(weighted, terms[1], PRECISE)
    products = []
    for p in range(NMOM):
        first_re, first_im = first[16 * p : 16 * p + 8], first[16 * p + 8 : 16 * p + 16]
        second_re, second_im = second[2 * p : 2 * p + 1], second[2 * p + 1 : 2 * p + 2]
        products.append(first_re * second_re - first_im * second_im)
        products.append(first_re * second_im + first_im * second_re)
    coeffs = dot_nt(jnp.concatenate(products, axis=0), terms[2], PRECISE)
    piece = jnp.concatenate([coeffs[8 * b : 8 * b + 8, 0:72] for b in range(8)] + [jnp.zeros((8, 64), F32)], axis=1)
    parity, pair = lax.rem(z, 2), z // 2
    pairs = chips // 2
    beside_z = z + 1 - 2 * parity
    gathered[core, parity, pair] = piece.astype(BF16)

    def send_far(i, carry):
        peer = lax.rem(pair + far_first(i, pairs), pairs)
        mine = gathered.at[core, parity, pair]
        remote(mine, mine, near_sem.at[0], ag_sem.at[pair], 2 * peer + parity, core).start()
        return carry

    lax.fori_loop(0, pairs - 1, send_far, 0)
    mine = gathered.at[core, parity, pair]
    remote(mine, mine, near_sem.at[1], side_sem, beside_z, core).start()

    def hand_on(i, carry):
        peer = lax.rem(pair + far_first(i, pairs), pairs)
        came = gathered.at[core, parity, peer]
        pltpu.make_async_copy(came, came, ag_sem.at[peer]).wait()
        remote(came, came, near_sem.at[1], side_sem, beside_z, core).start()
        return carry

    lax.fori_loop(0, pairs - 1, hand_on, 0)
    own = gathered.at[core, parity]
    own_to_core = remote(own, own, both_sem.at[0], both_sem.at[1], z, other)
    own_to_core.start()
    theirs = gathered.at[core, 1 - parity]
    pltpu.make_async_copy(theirs, theirs, side_sem).wait()
    theirs_to_core = remote(theirs, theirs, both_sem.at[2], both_sem.at[3], z, other)
    theirs_to_core.start()
    own_to_core.wait_recv()
    theirs_to_core.wait_recv()

    for h in range(2):
        for lb in range(5):
            lanes = slice(lb * LANES, (lb + 1) * LANES)
            tall = jnp.concatenate([gathered[h, zz % 2, zz // 2, :, lanes].astype(F32) for zz in range(chips)], axis=0)
            coeff_t[h, lanes] = tall.T
    for a in range(3):
        def rows_of(q, sign=1.0):
            taken = [
                coeff_t[h, (2 * p + q) * 72 + a * HALF : (2 * p + q) * 72 + (a + 1) * HALF]
                for p in range(NMOM)
                for h in range(2)
            ]
            return (sign * jnp.concatenate(taken, axis=0)).astype(BF16)

        left[a, 0:192, 0:NVEC] = rows_of(0)
        left[a, 0:192, NVEC:] = rows_of(1, -1.0)
        left[a, 192:384, 0:NVEC] = rows_of(1)
        left[a, 192:384, NVEC:] = rows_of(0)

    cos_z, sin_z = chip_phase[z, 0:1, 0:1], chip_phase[z, 1:2, 0:1]
    groups = length // GROUP
    my_group = me // 8

    def rebuild(i, carry):
        g = lax.rem(my_group + jnp.where(i == groups - 1, 0, far_first(i, groups)), groups)
        columns = pl.ds(pl.multiple_of(g * GROUP, GROUP), GROUP)
        table = phase_p[:, columns]
        cos_x, sin_x, cos_y, sin_y = (table[n : n + 1] for n in range(4))
        for a in range(3):
            result = dot(left[a], eig_p[a, :, columns])
            re = [result[48 * p : 48 * p + 48] for p in range(NMOM)]
            im = [result[192 + 48 * p : 240 + 48 * p] for p in range(NMOM)]
            out_re = re[0] + (cos_x * re[1] - sin_x * im[1]) + (cos_y * re[2] - sin_y * im[2]) + (cos_z * re[3] - sin_z * im[3])
            out_im = im[0] + (cos_x * im[1] + sin_x * re[1]) + (cos_y * im[2] + sin_y * re[2]) + (cos_z * im[3] + sin_z * re[3])
            source[48 * a : 48 * a + 48] = out_re * scale_out
            source[144 + 48 * a : 192 + 48 * a] = out_im * scale_out
        for k in range(2):
            tiles = [source[72 * q : 72 * q + 72, k * LANES : (k + 1) * LANES] for q in range(4)]
            for n, message in enumerate(swap_blocks(tiles, lane_blocks())):
                to_send[g * 8 + 4 * k + n] = message.reshape(9, 8, LANES).astype(BF16)
        for n in range(8):
            peer = g * 8 + n

            @pl.when(peer != me)
            def _():
                remote(to_send.at[peer], out.at[me], all_sem.at[0], all_sem.at[1], peer // 2, lax.rem(peer, 2)).start()

        return carry

    lax.fori_loop(0, groups, rebuild, 0)
    keep = pltpu.make_async_copy(to_send.at[me], out.at[me], all_sem.at[2])
    keep.start()

    def drain(ref, sem):
        pltpu.make_async_copy(ref, ref, sem).wait()

    drain(idx_rows.at[pl.ds(0, devices - 1)], idx_sem.at[0])
    drain(rs_send.at[pl.ds(0, chips - 1)], rs_sem.at[0])
    drain(gathered.at[0, 0, pl.ds(0, pairs - 1)], near_sem.at[0])
    drain(gathered.at[0, 0], near_sem.at[1])
    own_to_core.wait_send()
    theirs_to_core.wait_send()
    drain(to_send.at[pl.ds(0, devices - 1)], all_sem.at[0])
    keep.wait()
    drain(out.at[pl.ds(0, devices - 1)], all_sem.at[1])


def format_kernel(inp, out):
    lane_block = lane_blocks()
    for k in range(inp.shape[0] // 4):
        tiles = [inp[4 * k + d].astype(F32).reshape(72, LANES) for d in range(4)]
        rows = jnp.concatenate(swap_blocks(tiles, lane_block), axis=0)
        for q in range(2):
            for a in range(3):
                base = q * 144 + a * 48
                for s in range(4):
                    low = rows[base + 6 * s : base + 6 * s + 6]
                    high = rows[base + HALF + 6 * s : base + HALF + 6 * s + 6]
                    out[q, a, s, :, k * LANES : (k + 1) * LANES] = jnp.concatenate([low, high], axis=0).astype(BF16)


def on_device(propagator, eigvecs, operator_weights, sink_time, term_index, term_sign, solver_order):
    length = propagator.shape[-1]
    chips = lax.axis_size("space_0")
    devices = lax.axis_size(SPACE)
    pair = length // devices
    scale_in = 1.0 / math.sqrt(3.0 * length * devices)
    scale_out = 1.0 / math.sqrt(NMOM * NVEC)
    tables, pieces, chip_phase, pick, fold = fixed_tables(length, chips)
    weights = lax.dynamic_index_in_dim(operator_weights, sink_time[0], 0, keepdims=False)
    weights = jnp.pad(weights, ((0, 6), (0, 0)))
    terms = term_matrices(term_index, term_sign)
    me = lax.axis_index(SPACE)
    lane = jnp.arange(LANES, dtype=jnp.int32)
    idx_rows = jnp.where(lane // pair == me % 4, jnp.tile(solver_order.reshape(devices, pair), (1, 4)), 0)
    idx_rows = idx_rows.reshape(devices, 1, LANES)

    vmem = pl.BlockSpec(memory_space=pltpu.VMEM)
    hbm = pl.BlockSpec(memory_space=pl.ANY)
    arrived = pl.pallas_call(
        functools.partial(whole_kernel, chips, length, scale_in, scale_out),
        out_shape=jax.ShapeDtypeStruct((devices, 9, 8, LANES), BF16),
        in_specs=[hbm, hbm] + [vmem] * 8,
        out_specs=hbm,
        scratch_shapes=[
            pltpu.VMEM((3, 2 * NVEC, length), BF16),
            pltpu.VMEM((2, 3, 4, 12, length), BF16),
            pltpu.VMEM((2, 3, NVEC, 144), F32),
            pltpu.VMEM((2, NVEC, 512), F32),
            pltpu.VMEM((NVEC, 512), F32),
            pltpu.VMEM((NVEC, 512), F32),
            pltpu.VMEM((chips, 8, 512), BF16),
            pltpu.VMEM((chips, 8, 512), BF16),
            pltpu.VMEM((devices, 1, LANES), jnp.int32),
            pltpu.VMEM((length, GROUP), BF16),
            pltpu.VMEM((3, 2 * NVEC, length), BF16),
            pltpu.VMEM((8, length), F32),
            pltpu.VMEM((2, 2, chips // 2, 8, 640), BF16),
            pltpu.VMEM((2, 640, NVEC), F32),
            pltpu.VMEM((3, 384, 2 * NVEC), BF16),
            pltpu.VMEM((288, GROUP), F32),
            pltpu.VMEM((devices, 9, 8, LANES), BF16),
            pltpu.SemaphoreType.DMA((12,)),
            pltpu.SemaphoreType.DMA((2,)),
            pltpu.SemaphoreType.DMA((2,)),
            pltpu.SemaphoreType.DMA((2,)),
            pltpu.SemaphoreType.DMA((2,)),
            pltpu.SemaphoreType.DMA((chips // 2,)),
            pltpu.SemaphoreType.DMA,
            pltpu.SemaphoreType.DMA((4,)),
            pltpu.SemaphoreType.DMA((3,)),
        ],
        compiler_params=pltpu.CompilerParams(collective_id=0, has_side_effects=True, vmem_limit_bytes=56 * 2**20),
    )(
        eigvecs, propagator, idx_rows, weights, jnp.asarray(tables), jnp.asarray(pieces),
        jnp.asarray(chip_phase), jnp.asarray(pick), jnp.asarray(fold), terms,
    )
    take = 16
    return pl.pallas_call(
        format_kernel,
        out_shape=jax.ShapeDtypeStruct((2, 3, 4, 12, length), BF16),
        grid=(devices // take,),
        in_specs=[pl.BlockSpec((take, 9, 8, LANES), lambda i: (i, 0, 0, 0))],
        out_specs=pl.BlockSpec((2, 3, 4, 12, take * pair), lambda i: (0, 0, 0, 0, i)),
    )(arrived)


def solution(mesh):
    finer = Mesh(mesh.devices.reshape(mesh.shape["grp"], -1, 2), ("grp", "space_0", "space_1"))
    in_specs = (
        P("grp", None, None, None, SPACE),
        P("grp", None, None, SPACE),
        P("grp", None, None),
        P("grp"),
        P(),
        P(),
        P(SPACE),
    )
    out_specs = P("grp", None, None, None, SPACE)
    return jax.shard_map(on_device, mesh=finer, in_specs=in_specs, out_specs=out_specs, check_vma=False)
```

```python
import functools
import math

import jax
import jax.numpy as jnp
import ml_dtypes
import numpy as np
from jax import lax
from jax.experimental import pallas as pl
from jax.experimental.pallas import tpu as pltpu
from jax.sharding import Mesh
from jax.sharding import PartitionSpec as P

NVEC = 256
NMOM = 4
NTERM = 48
EXTENT = 64
SPACE = ("space_0", "space_1")
MESH = pl.DeviceIdType.MESH
PRECISE = lax.Precision.HIGHEST
F32 = jnp.float32
BF16 = jnp.bfloat16

LANES = 128
HALF = 24
CHUNK = 512
GROUP = 256


def fixed_tables(length, chips):
    assert 2 * length == EXTENT * EXTENT
    site = np.arange(length)
    turn = 2.0 * np.pi / EXTENT
    angle_x = turn * (site % EXTENT)
    tables, pieces = [], []
    for core in range(2):
        angle_y = turn * ((core * length + site) // EXTENT % EXTENT)
        rows = np.stack([np.cos(angle_x), np.sin(angle_x), np.cos(angle_y), np.sin(angle_y)]).astype(np.float32)
        tables.append(np.concatenate([rows, np.zeros_like(rows)]))
        high = rows.astype(ml_dtypes.bfloat16)
        middle = (rows - high.astype(np.float32)).astype(ml_dtypes.bfloat16)
        low = (rows - high.astype(np.float32) - middle.astype(np.float32)).astype(ml_dtypes.bfloat16)
        pieces.append(np.concatenate([high, middle, low, np.zeros_like(high)]))
    angle_z = turn * (np.arange(chips) % EXTENT)
    chip_phase = np.zeros((chips, 8, LANES), np.float32)
    chip_phase[:, 0] = np.cos(angle_z)[:, None]
    chip_phase[:, 1] = np.sin(angle_z)[:, None]
    pick = np.zeros((2, 8, 512), np.float32)
    fold = np.zeros((2, 512, LANES), np.float32)
    for colour in range(3):
        for row in range(6):
            for u in range(HALF):
                lane = colour * 144 + row * HALF + u
                pick[0, row, lane] = 1.0
                pick[1, row ^ 1, lane] = 1.0 if row % 2 == 0 else -1.0
                fold[0, lane, colour * HALF + u] = 1.0
                fold[1, lane, 48 + colour * HALF + u] = 1.0
    return np.stack(tables), np.stack(pieces), chip_phase, pick, fold


def term_matrices(index, sign):
    shape = (LANES, 384)
    row = lax.broadcasted_iota(jnp.int32, shape, 0)
    column = lax.broadcasted_iota(jnp.int32, shape, 1) // 64
    same = (row % HALF // 4 == column) & (row < 72)
    channel = row // HALF * 4 + row % 4

    def along(values, rest):
        one = jnp.concatenate([values, jnp.full((1, 64 - NTERM), rest, values.dtype)], axis=1)
        return jnp.concatenate([one] * 6, axis=1)

    picks = [jnp.where(same & (channel == along(index[n : n + 1], -1)), 1.0, 0.0) for n in range(3)]
    signs = (2 * along(sign, 0) - 1).astype(F32)
    return picks[0], picks[1], picks[2] * signs


def dot(a, b, precision=None):
    return lax.dot_general(a, b, (((1,), (0,)), ((), ())), preferred_element_type=F32, precision=precision)


def dot_nt(a, b, precision=None):
    return lax.dot_general(a, b, (((1,), (1,)), ((), ())), preferred_element_type=F32, precision=precision)


def far_first(step, count):
    half = (step + 1) // 2
    return count // 2 + half * (1 - 2 * (step % 2))


def swap_blocks(tiles, lane_block):
    result = []
    for g in range(4):
        message = tiles[0] if g == 0 else pltpu.roll(tiles[0], (-g * 32) % LANES, 1)
        for q in range(1, 4):
            moved = tiles[q] if q == g else pltpu.roll(tiles[q], ((q - g) * 32) % LANES, 1)
            message = jnp.where(lane_block == q, moved, message)
        result.append(message)
    return result


def lane_blocks():
    return lax.broadcasted_iota(jnp.int32, (72, LANES), 1) // 32


def whole_kernel(
    chips, length, scale_in, scale_out,
    eig, prop, op_weights, sink, order, index, sign, tables, pieces, chip_phase, pick, fold,
    out,
    eig_v, prop_v, weights_v, sink_v, order_v, index_v, sign_v, tables_v, pieces_v, phase_v, pick_v, fold_v,
    accs, full, from_core, chip_sum, rs_send, rs_recv, idx_send, idx_recv, terms,
    perm, eig_p, phase_p, gathered, coeff_t, left, source, to_send, arrived, result,
    load_sem, table_sem, core_sem, idx_sem, rs_sem, near_sem, ag_sem, side_sem, both_send, both_sem, all_send, all_sem, out_sem,
):
    z = lax.axis_index("space_0")
    core = lax.axis_index("space_1")
    devices = 2 * chips
    me = 2 * z + core
    other = 1 - core

    def device(chip, on_core):
        return {"space_0": chip, "space_1": on_core}

    def remote(src, dst, send_sem, recv_sem, chip, on_core):
        return pltpu.make_async_remote_copy(
            src_ref=src, dst_ref=dst, send_sem=send_sem, recv_sem=recv_sem,
            device_id=device(chip, on_core), device_id_type=MESH,
        )

    loads = []
    for a in range(3):
        for q in range(2):
            loads.append(pltpu.make_async_copy(prop.at[q, a], prop_v.at[q, a], load_sem.at[4 * a + q]))
            loads.append(pltpu.make_async_copy(eig.at[q, a], eig_v.at[a, pl.ds(q * NVEC, NVEC)], load_sem.at[4 * a + 2 + q]))
    table_load = pltpu.make_async_copy(tables.at[core], tables_v, table_sem.at[0])
    late_loads = [
        pltpu.make_async_copy(op_weights, weights_v, table_sem.at[1]),
        pltpu.make_async_copy(pick, pick_v, table_sem.at[2]),
        pltpu.make_async_copy(fold, fold_v, table_sem.at[3]),
        pltpu.make_async_copy(pieces.at[core], pieces_v, table_sem.at[4]),
        pltpu.make_async_copy(chip_phase, phase_v, table_sem.at[5]),
        pltpu.make_async_copy(sink, sink_v, table_sem.at[6]),
        pltpu.make_async_copy(index, index_v, table_sem.at[7]),
        pltpu.make_async_copy(sign, sign_v, table_sem.at[8]),
        pltpu.make_async_copy(order, order_v, table_sem.at[9]),
    ]
    for load in [table_load] + loads + late_loads:
        load.start()

    barrier = pltpu.get_barrier_semaphore()

    def signal(chip, on_core):
        pl.semaphore_signal(barrier, inc=1, device_id=device(chip, on_core), device_id_type=MESH)

    def greet(i, carry):
        peer = lax.rem(z + far_first(i, chips), chips)
        signal(peer, 0)
        signal(peer, 1)
        return carry

    lax.fori_loop(0, chips - 1, greet, 0)
    signal(z, other)
    table_load.wait()

    for a in range(3):
        for load in loads[4 * a : 4 * a + 4]:
            load.wait()
        for h in range(2):
            accs[h, a] = jnp.zeros((NVEC, 144), F32)

        def project(ci, carry, a=a):
            sites = pl.ds(pl.multiple_of(ci * CHUNK, CHUNK), CHUNK)
            table = tables_v[:, sites]
            cos_x, sin_x, cos_y, sin_y = (table[n : n + 1] for n in range(4))
            real = prop_v[0, a, :, :, sites].astype(F32)
            imag = prop_v[1, a, :, :, sites].astype(F32)
            for h in range(2):
                re = real[6 * h : 6 * h + 6].reshape(HALF, CHUNK)
                im = imag[6 * h : 6 * h + 6].reshape(HALF, CHUNK)
                re_x, im_x = cos_x * re + sin_x * im, cos_x * im - sin_x * re
                re_y, im_y = cos_y * re + sin_y * im, cos_y * im - sin_y * re
                with_real = jnp.concatenate([re, im, re_x, im_x, re_y, im_y], axis=0).astype(BF16)
                with_imag = jnp.concatenate([im, -re, im_x, -re_x, im_y, -re_y], axis=0).astype(BF16)
                accs[h, a] += dot_nt(eig_v[a, 0:NVEC, sites], with_real) + dot_nt(eig_v[a, NVEC : 2 * NVEC, sites], with_imag)
            return carry

        lax.fori_loop(0, length // CHUNK, project, 0)

    def join_colours(rb, carry):
        rows = pl.ds(pl.multiple_of(rb * 32, 32), 32)
        for h in range(2):
            full[h, rows] = jnp.concatenate([accs[h, a, rows] for a in range(3)] + [jnp.zeros((32, 80), F32)], axis=1)
        return carry

    lax.fori_loop(0, NVEC // 32, join_colours, 0)

    for load in late_loads:
        load.wait()

    lane_block = lax.broadcasted_iota(jnp.int32, (devices // 4, LANES), 1) // 32
    my_block = lax.rem(me, 4)
    for k in range(4):
        moved = jnp.zeros((devices // 4, LANES), jnp.int32)
        for t in range(4):
            turned = order_v[...] if t == k else pltpu.roll(order_v[...], ((t - k) * 32) % LANES, 1)
            moved = jnp.where((lane_block == t) & (my_block == t), turned, moved)
        idx_send[k] = moved.reshape(devices // 4, 1, LANES)
    for n, matrix in enumerate(term_matrices(index_v[...], sign_v[...])):
        terms[n] = matrix
    pl.semaphore_wait(barrier, devices - 1)

    to_core = remote(full.at[other], from_core, core_sem.at[0], core_sem.at[1], z, other)
    to_core.start()

    def send_index(i, carry):
        peer = lax.rem(z + far_first(i, chips), chips)
        for n in range(2):
            mine = idx_send.at[2 * lax.rem(peer, 2) + n, peer // 2]
            remote(mine, idx_recv.at[me], idx_sem.at[0], idx_sem.at[1], peer, n).start()
        return carry

    lax.fori_loop(0, chips - 1, send_index, 0)
    remote(idx_send.at[2 * lax.rem(z, 2) + other, z // 2], idx_recv.at[me], idx_sem.at[0], idx_sem.at[1], z, other).start()
    idx_recv[me] = idx_send[my_block, z // 2]

    to_core.wait()
    chip_sum[...] = (full[core] + from_core[...]) * scale_in

    times = lax.broadcasted_iota(jnp.int32, weights_v.shape, 0)
    weights = jnp.sum(jnp.where(times == sink_v[...].reshape(1, 1, 1), weights_v[...], 0.0), axis=0)
    weights = jnp.concatenate([weights, jnp.zeros((6, NVEC), F32)], axis=0)
    by_weight = dot(weights, chip_sum[...], PRECISE)
    weighted_rows = by_weight[0:1] * pick_v[0] + by_weight[1:2] * pick_v[1]
    weighted_part = dot(weighted_rows, fold_v[1], PRECISE)
    beside = jnp.concatenate([jnp.zeros((8, 384), F32), weighted_part], axis=1)

    def pack(zz, carry):
        rows = pl.ds(pl.multiple_of(zz * 8, 8), 8)
        rs_send[zz] = (chip_sum[rows] + beside).astype(BF16)
        return carry

    lax.fori_loop(0, chips, pack, 0)

    def send_part(i, carry):
        peer = lax.rem(z + far_first(i, chips), chips)
        remote(rs_send.at[peer], rs_recv.at[z], rs_sem.at[0], rs_sem.at[1], peer, core).start()
        return carry

    lax.fori_loop(0, chips - 1, send_part, 0)
    rs_recv[z] = rs_send[z]

    some = pl.ds(0, devices - 1)
    pltpu.make_async_copy(idx_recv.at[some], idx_recv.at[some], idx_sem.at[1]).wait()

    def reorder(g, carry):
        columns = pl.ds(pl.multiple_of(g * GROUP, GROUP), GROUP)
        wanted = jnp.concatenate(
            [sum(idx_recv[g * 8 + 4 * k + n] for n in range(4)) for k in range(2)], axis=1
        ) - me * length

        def one_hot(rb, inner):
            rows = pl.ds(pl.multiple_of(rb * 64, 64), 64)
            here = lax.broadcasted_iota(jnp.int32, (64, GROUP), 0) + rb * 64
            perm[rows] = jnp.where(here == wanted, 1.0, 0.0).astype(BF16)
            return inner

        lax.fori_loop(0, length // 64, one_hot, 0)
        for a in range(3):
            eig_p[a, :, columns] = dot(eig_v[a], perm[...]).astype(BF16)
        turned = dot(pieces_v[...], perm[...])
        phase_p[:, columns] = jnp.concatenate([turned[0:4] + turned[4:8] + turned[8:12], jnp.zeros((4, GROUP), F32)], axis=0)
        return carry

    lax.fori_loop(0, length // GROUP, reorder, 0)

    some = pl.ds(0, chips - 1)
    pltpu.make_async_copy(rs_recv.at[some], rs_recv.at[some], rs_sem.at[1]).wait()
    total = jnp.zeros((8, 512), F32)
    total_cos = jnp.zeros((8, 512), F32)
    total_sin = jnp.zeros((8, 512), F32)
    for zz in range(chips):
        part = rs_recv[zz].astype(F32)
        total = total + part
        total_cos = total_cos + phase_v[zz, 0:1, 0:1] * part
        total_sin = total_sin + phase_v[zz, 1:2, 0:1] * part
    masks = pick_v[0]
    blocks = [total * masks[r : r + 1] for r in range(6)]
    blocks.append(total_cos * masks[0:1] + total_sin * masks[1:2])
    blocks.append(total_cos * masks[1:2] - total_sin * masks[0:1])
    block_rows = dot(jnp.concatenate(blocks, axis=0), fold_v[0], PRECISE)
    tails = [pltpu.roll(t[:, 384:512], LANES - 48, 1) for t in (total, total_cos, total_sin)]
    weighted = jnp.concatenate(
        [tails[0][0:6], tails[1][0:1] + tails[2][1:2], tails[1][1:2] - tails[2][0:1]], axis=0
    )
    first = dot(block_rows, terms[0], PRECISE)
    second = dot(weighted, terms[1], PRECISE)
    products = []
    for p in range(NMOM):
        first_re, first_im = first[16 * p : 16 * p + 8], first[16 * p + 8 : 16 * p + 16]
        second_re, second_im = second[2 * p : 2 * p + 1], second[2 * p + 1 : 2 * p + 2]
        products.append(first_re * second_re - first_im * second_im)
        products.append(first_re * second_im + first_im * second_re)
    coeffs = dot_nt(jnp.concatenate(products, axis=0), terms[2], PRECISE)
    piece = jnp.concatenate([coeffs[8 * b : 8 * b + 8, 0:72] for b in range(8)] + [jnp.zeros((8, 64), F32)], axis=1)
    member, quad = lax.rem(z, 4), z // 4
    quads = chips // 4
    gathered[core, member, quad] = piece.astype(BF16)

    def send_far(i, carry):
        peer = lax.rem(quad + far_first(i, quads), quads)
        mine = gathered.at[core, member, quad]
        remote(mine, mine, near_sem.at[0], ag_sem.at[quad], 4 * peer + member, core).start()
        return carry

    lax.fori_loop(0, quads - 1, send_far, 0)

    def spread(came):
        for o in (2, 1, 3):
            remote(came, came, near_sem.at[1], side_sem.at[member], 4 * quad + lax.rem(member + o, 4), core).start()

    spread(gathered.at[core, member, quad])

    def hand_on(i, carry):
        peer = lax.rem(quad + far_first(quads - 2 - i, quads), quads)
        came = gathered.at[core, member, peer]
        pltpu.make_async_copy(came, came, ag_sem.at[peer]).wait()
        spread(came)
        return carry

    lax.fori_loop(0, quads - 1, hand_on, 0)
    for o in range(4):
        whose = lax.rem(member + o, 4)
        theirs = gathered.at[core, whose]
        if o:
            pltpu.make_async_copy(theirs, theirs, side_sem.at[whose]).wait()
        remote(theirs, theirs, both_send, both_sem.at[whose], z, other).start()
    for o in range(4):
        theirs = gathered.at[other, o]
        pltpu.make_async_copy(theirs, theirs, both_sem.at[o]).wait()

    for h in range(2):
        for lb in range(5):
            lanes = slice(lb * LANES, (lb + 1) * LANES)
            tall = jnp.concatenate([gathered[h, zz % 4, zz // 4, :, lanes].astype(F32) for zz in range(chips)], axis=0)
            coeff_t[h, lanes] = tall.T
    for a in range(3):
        def rows_of(q, sign=1.0):
            taken = [
                coeff_t[h, (2 * p + q) * 72 + a * HALF : (2 * p + q) * 72 + (a + 1) * HALF]
                for p in range(NMOM)
                for h in range(2)
            ]
            return (sign * jnp.concatenate(taken, axis=0)).astype(BF16)

        left[a, 0:192, 0:NVEC] = rows_of(0)
        left[a, 0:192, NVEC:] = rows_of(1, -1.0)
        left[a, 192:384, 0:NVEC] = rows_of(1)
        left[a, 192:384, NVEC:] = rows_of(0)

    cos_z, sin_z = phase_v[z, 0:1, 0:1], phase_v[z, 1:2, 0:1]
    groups = length // GROUP
    my_group = me // 8

    def rebuild(i, carry):
        g = lax.rem(my_group + jnp.where(i == groups - 1, 0, far_first(i, groups)), groups)
        columns = pl.ds(pl.multiple_of(g * GROUP, GROUP), GROUP)
        table = phase_p[:, columns]
        cos_x, sin_x, cos_y, sin_y = (table[n : n + 1] for n in range(4))
        for a in range(3):
            both = dot(left[a], eig_p[a, :, columns])
            re = [both[48 * p : 48 * p + 48] for p in range(NMOM)]
            im = [both[192 + 48 * p : 240 + 48 * p] for p in range(NMOM)]
            out_re = re[0] + (cos_x * re[1] - sin_x * im[1]) + (cos_y * re[2] - sin_y * im[2]) + (cos_z * re[3] - sin_z * im[3])
            out_im = im[0] + (cos_x * im[1] + sin_x * re[1]) + (cos_y * im[2] + sin_y * re[2]) + (cos_z * im[3] + sin_z * re[3])
            source[48 * a : 48 * a + 48] = out_re * scale_out
            source[144 + 48 * a : 192 + 48 * a] = out_im * scale_out
        for k in range(2):
            tiles = [source[72 * q : 72 * q + 72, k * LANES : (k + 1) * LANES] for q in range(4)]
            for n, message in enumerate(swap_blocks(tiles, lane_blocks())):
                to_send[g * 8 + 4 * k + n] = message.reshape(9, 8, LANES).astype(BF16)
        for n in range(8):
            peer = g * 8 + n

            @pl.when(peer != me)
            def _():
                remote(to_send.at[peer], arrived.at[me], all_send, all_sem.at[z // 2], peer // 2, n % 2).start()

        return carry

    lax.fori_loop(0, groups, rebuild, 0)
    arrived[me] = to_send[me]

    source_pairs = chips // 2

    def place(group):
        tiles = [arrived[4 * group + d].astype(F32).reshape(72, LANES) for d in range(4)]
        rows = jnp.concatenate(swap_blocks(tiles, lane_blocks()), axis=0)
        columns = pl.ds(pl.multiple_of(group * LANES, LANES), LANES)
        for q in range(2):
            for a in range(3):
                base = q * 144 + a * 48
                result[q, a, :, :, columns] = rows[base : base + 48].reshape(12, 4, LANES).astype(BF16)
        pltpu.make_async_copy(result.at[:, :, :, :, columns], out.at[:, :, :, :, columns], out_sem).start()

    def finish(i, carry):
        group = lax.rem(z // 2 + far_first(i, source_pairs), source_pairs)
        four = arrived.at[pl.ds(4 * group, 4)]
        pltpu.make_async_copy(four, four, all_sem.at[group]).wait()
        place(group)
        return carry

    lax.fori_loop(0, source_pairs - 1, finish, 0)
    three = arrived.at[pl.ds(0, 3)]
    pltpu.make_async_copy(three, three, all_sem.at[z // 2]).wait()
    place(z // 2)

    def drain(ref, sem):
        pltpu.make_async_copy(ref, ref, sem).wait()

    drain(idx_recv.at[pl.ds(0, devices - 1)], idx_sem.at[0])
    drain(rs_send.at[pl.ds(0, chips - 1)], rs_sem.at[0])
    drain(gathered.at[0, 0, pl.ds(0, quads - 1)], near_sem.at[0])
    drain(gathered.at[0, pl.ds(0, 3)], near_sem.at[1])
    drain(gathered.at[0], both_send)
    drain(to_send.at[pl.ds(0, devices - 1)], all_send)
    drain(result, out_sem)


def on_device(propagator, eigvecs, operator_weights, sink_time, term_index, term_sign, solver_order):
    length = propagator.shape[-1]
    chips = lax.axis_size("space_0")
    devices = lax.axis_size(SPACE)
    scale_in = 1.0 / math.sqrt(3.0 * length * devices)
    scale_out = 1.0 / math.sqrt(NMOM * NVEC)
    tables, pieces, chip_phase, pick, fold = fixed_tables(length, chips)
    hbm = pl.BlockSpec(memory_space=pl.ANY)
    arrived = pltpu.VMEM((devices, 9, 8, LANES), BF16)
    result = pl.pallas_call(
        functools.partial(whole_kernel, chips, length, scale_in, scale_out),
        out_shape=jax.ShapeDtypeStruct((2, 3, 12, 4, length), BF16),
        in_specs=[hbm] * 12,
        out_specs=hbm,
        scratch_shapes=[
            pltpu.VMEM((3, 2 * NVEC, length), BF16),
            pltpu.VMEM((2, 3, 12, 4, length), BF16),
            pltpu.VMEM(operator_weights.shape, F32),
            pltpu.VMEM((1, 1), jnp.int32),
            pltpu.VMEM((devices // 4, LANES), jnp.int32),
            pltpu.VMEM((3, NTERM), jnp.int32),
            pltpu.VMEM((1, NTERM), jnp.int32),
            pltpu.VMEM(tables.shape[1:], F32),
            pltpu.VMEM(pieces.shape[1:], BF16),
            pltpu.VMEM(chip_phase.shape, F32),
            pltpu.VMEM(pick.shape, F32),
            pltpu.VMEM(fold.shape, F32),
            pltpu.VMEM((2, 3, NVEC, 144), F32),
            pltpu.VMEM((2, NVEC, 512), F32),
            pltpu.VMEM((NVEC, 512), F32),
            pltpu.VMEM((NVEC, 512), F32),
            pltpu.VMEM((chips, 8, 512), BF16),
            pltpu.VMEM((chips, 8, 512), BF16),
            pltpu.VMEM((4, devices // 4, 1, LANES), jnp.int32),
            pltpu.VMEM((devices, 1, LANES), jnp.int32),
            pltpu.VMEM((3, LANES, 384), F32),
            pltpu.VMEM((length, GROUP), BF16),
            pltpu.VMEM((3, 2 * NVEC, length), BF16),
            pltpu.VMEM((8, length), F32),
            pltpu.VMEM((2, 4, chips // 4, 8, 640), BF16),
            pltpu.VMEM((2, 640, NVEC), F32),
            pltpu.VMEM((3, 384, 2 * NVEC), BF16),
            pltpu.VMEM((288, GROUP), F32),
            arrived,
            arrived,
            pltpu.VMEM((2, 3, 12, 4, length), BF16),
            pltpu.SemaphoreType.DMA((12,)),
            pltpu.SemaphoreType.DMA((10,)),
            pltpu.SemaphoreType.DMA((2,)),
            pltpu.SemaphoreType.DMA((2,)),
            pltpu.SemaphoreType.DMA((2,)),
            pltpu.SemaphoreType.DMA((2,)),
            pltpu.SemaphoreType.DMA((chips // 4,)),
            pltpu.SemaphoreType.DMA((4,)),
            pltpu.SemaphoreType.DMA,
            pltpu.SemaphoreType.DMA((4,)),
            pltpu.SemaphoreType.DMA,
            pltpu.SemaphoreType.DMA((chips // 2,)),
            pltpu.SemaphoreType.DMA,
        ],
        compiler_params=pltpu.CompilerParams(collective_id=0, has_side_effects=True, vmem_limit_bytes=56 * 2**20),
    )(
        eigvecs, jnp.swapaxes(propagator, 2, 3), operator_weights, sink_time.reshape(1, 1), solver_order.reshape(devices // 4, LANES),
        term_index.T, term_sign.reshape(1, -1), jnp.asarray(tables), jnp.asarray(pieces), jnp.asarray(chip_phase),
        jnp.asarray(pick), jnp.asarray(fold),
    )
    return jnp.swapaxes(result, 2, 3)


def solution(mesh):
    finer = Mesh(mesh.devices.reshape(mesh.shape["grp"], -1, 2), ("grp", "space_0", "space_1"))
    in_specs = (
        P("grp", None, None, None, SPACE),
        P("grp", None, None, SPACE),
        P("grp", None, None),
        P("grp"),
        P(),
        P(),
        P(SPACE),
    )
    out_specs = P("grp", None, None, None, SPACE)
    return jax.shard_map(on_device, mesh=finer, in_specs=in_specs, out_specs=out_specs, check_vma=False)
```

```python
import functools
import math

import jax
import jax.numpy as jnp
import ml_dtypes
import numpy as np
from jax import lax
from jax.experimental import pallas as pl
from jax.experimental.pallas import tpu as pltpu
from jax.sharding import Mesh
from jax.sharding import PartitionSpec as P

NVEC = 256
NMOM = 4
NTERM = 48
EXTENT = 64
SPACE = ("space_0", "space_1")
MESH = pl.DeviceIdType.MESH
PRECISE = lax.Precision.HIGHEST
F32 = jnp.float32
BF16 = jnp.bfloat16

LANES = 128
HALF = 24
CHUNK = 512
GROUP = 256


def fixed_tables(length, chips):
    assert 2 * length == EXTENT * EXTENT
    site = np.arange(length)
    turn = 2.0 * np.pi / EXTENT
    angle_x = turn * (site % EXTENT)
    tables, pieces = [], []
    for core in range(2):
        angle_y = turn * ((core * length + site) // EXTENT % EXTENT)
        rows = np.stack([np.cos(angle_x), np.sin(angle_x), np.cos(angle_y), np.sin(angle_y)]).astype(np.float32)
        tables.append(np.concatenate([rows, np.zeros_like(rows)]))
        high = rows.astype(ml_dtypes.bfloat16)
        middle = (rows - high.astype(np.float32)).astype(ml_dtypes.bfloat16)
        low = (rows - high.astype(np.float32) - middle.astype(np.float32)).astype(ml_dtypes.bfloat16)
        pieces.append(np.concatenate([high, middle, low, np.zeros_like(high)]))
    angle_z = turn * (np.arange(chips) % EXTENT)
    chip_phase = np.zeros((chips, 8, LANES), np.float32)
    chip_phase[:, 0] = np.cos(angle_z)[:, None]
    chip_phase[:, 1] = np.sin(angle_z)[:, None]
    pick = np.zeros((2, 8, 512), np.float32)
    fold = np.zeros((2, 512, LANES), np.float32)
    for colour in range(3):
        for row in range(6):
            for u in range(HALF):
                lane = colour * 144 + row * HALF + u
                pick[0, row, lane] = 1.0
                pick[1, row ^ 1, lane] = 1.0 if row % 2 == 0 else -1.0
                fold[0, lane, colour * HALF + u] = 1.0
                fold[1, lane, 48 + colour * HALF + u] = 1.0
    return np.stack(tables), np.stack(pieces), chip_phase, pick, fold


def term_matrices(index, sign):
    shape = (LANES, 384)
    row = lax.broadcasted_iota(jnp.int32, shape, 0)
    column = lax.broadcasted_iota(jnp.int32, shape, 1) // 64
    same = (row % HALF // 4 == column) & (row < 72)
    channel = row // HALF * 4 + row % 4

    def along(values, rest):
        one = jnp.concatenate([values, jnp.full((1, 64 - NTERM), rest, values.dtype)], axis=1)
        return jnp.concatenate([one] * 6, axis=1)

    picks = [jnp.where(same & (channel == along(index[n : n + 1], -1)), 1.0, 0.0) for n in range(3)]
    signs = (2 * along(sign, 0) - 1).astype(F32)
    return picks[0], picks[1], picks[2] * signs


def dot(a, b, precision=None):
    return lax.dot_general(a, b, (((1,), (0,)), ((), ())), preferred_element_type=F32, precision=precision)


def dot_nt(a, b, precision=None):
    return lax.dot_general(a, b, (((1,), (1,)), ((), ())), preferred_element_type=F32, precision=precision)


def far_first(step, count):
    half = (step + 1) // 2
    return count // 2 + half * (1 - 2 * (step % 2))


def swap_blocks(tiles, lane_block):
    result = []
    for g in range(4):
        message = tiles[0] if g == 0 else pltpu.roll(tiles[0], (-g * 32) % LANES, 1)
        for q in range(1, 4):
            moved = tiles[q] if q == g else pltpu.roll(tiles[q], ((q - g) * 32) % LANES, 1)
            message = jnp.where(lane_block == q, moved, message)
        result.append(message)
    return result


def lane_blocks():
    return lax.broadcasted_iota(jnp.int32, (72, LANES), 1) // 32


def whole_kernel(
    chips, length, scale_in, scale_out,
    eig, prop, op_weights, sink, order, index, sign, tables, pieces, chip_phase, pick, fold,
    out,
    eig_v, prop_v, weights_v, sink_v, order_v, index_v, sign_v, tables_v, pieces_v, phase_v, pick_v, fold_v,
    accs, full, from_core, chip_sum, rs_send, rs_recv, idx_send, idx_recv, terms,
    perm, eig_p, phase_p, gathered, coeff_t, left, source, to_send, arrived, result,
    load_sem, table_sem, core_sem, idx_sem, rs_sem, near_sem, ag_sem, side_sem, both_send, both_sem, all_send, all_sem, out_sem,
):
    z = lax.axis_index("space_0")
    core = lax.axis_index("space_1")
    devices = 2 * chips
    me = 2 * z + core
    other = 1 - core

    def device(chip, on_core):
        return {"space_0": chip, "space_1": on_core}

    def remote(src, dst, send_sem, recv_sem, chip, on_core):
        return pltpu.make_async_remote_copy(
            src_ref=src, dst_ref=dst, send_sem=send_sem, recv_sem=recv_sem,
            device_id=device(chip, on_core), device_id_type=MESH,
        )

    loads = []
    for a in range(3):
        for q in range(2):
            loads.append(pltpu.make_async_copy(prop.at[q, a], prop_v.at[q, a], load_sem.at[4 * a + q]))
            loads.append(pltpu.make_async_copy(eig.at[q, a], eig_v.at[a, pl.ds(q * NVEC, NVEC)], load_sem.at[4 * a + 2 + q]))
    table_load = pltpu.make_async_copy(tables.at[core], tables_v, table_sem.at[0])
    late_loads = [
        pltpu.make_async_copy(op_weights, weights_v, table_sem.at[1]),
        pltpu.make_async_copy(pick, pick_v, table_sem.at[2]),
        pltpu.make_async_copy(fold, fold_v, table_sem.at[3]),
        pltpu.make_async_copy(pieces.at[core], pieces_v, table_sem.at[4]),
        pltpu.make_async_copy(chip_phase, phase_v, table_sem.at[5]),
        pltpu.make_async_copy(sink, sink_v, table_sem.at[6]),
        pltpu.make_async_copy(index, index_v, table_sem.at[7]),
        pltpu.make_async_copy(sign, sign_v, table_sem.at[8]),
        pltpu.make_async_copy(order, order_v, table_sem.at[9]),
    ]
    for load in [table_load] + loads + late_loads:
        load.start()

    barrier = pltpu.get_barrier_semaphore()

    def signal(chip, on_core):
        pl.semaphore_signal(barrier, inc=1, device_id=device(chip, on_core), device_id_type=MESH)

    def greet(i, carry):
        peer = lax.rem(z + far_first(i, chips), chips)
        signal(peer, 0)
        signal(peer, 1)
        return carry

    lax.fori_loop(0, chips - 1, greet, 0)
    signal(z, other)
    table_load.wait()

    for a in range(3):
        for load in loads[4 * a : 4 * a + 4]:
            load.wait()
        for h in range(2):
            accs[h, a] = jnp.zeros((NVEC, 144), F32)

        def project(ci, carry, a=a):
            sites = pl.ds(pl.multiple_of(ci * CHUNK, CHUNK), CHUNK)
            table = tables_v[:, sites]
            cos_x, sin_x, cos_y, sin_y = (table[n : n + 1] for n in range(4))
            real = prop_v[0, a, :, :, sites].astype(F32)
            imag = prop_v[1, a, :, :, sites].astype(F32)
            for h in range(2):
                re = real[6 * h : 6 * h + 6].reshape(HALF, CHUNK)
                im = imag[6 * h : 6 * h + 6].reshape(HALF, CHUNK)
                re_x, im_x = cos_x * re + sin_x * im, cos_x * im - sin_x * re
                re_y, im_y = cos_y * re + sin_y * im, cos_y * im - sin_y * re
                with_real = jnp.concatenate([re, im, re_x, im_x, re_y, im_y], axis=0).astype(BF16)
                with_imag = jnp.concatenate([im, -re, im_x, -re_x, im_y, -re_y], axis=0).astype(BF16)
                accs[h, a] += dot_nt(eig_v[a, 0:NVEC, sites], with_real) + dot_nt(eig_v[a, NVEC : 2 * NVEC, sites], with_imag)
            return carry

        lax.fori_loop(0, length // CHUNK, project, 0)

    def join_colours(rb, carry):
        rows = pl.ds(pl.multiple_of(rb * 32, 32), 32)
        for h in range(2):
            full[h, rows] = jnp.concatenate([accs[h, a, rows] for a in range(3)] + [jnp.zeros((32, 80), F32)], axis=1)
        return carry

    lax.fori_loop(0, NVEC // 32, join_colours, 0)

    for load in late_loads:
        load.wait()

    for k in range(4):
        idx_send[k] = order_v[:, 32 * k : 32 * k + 32].reshape(devices // 4, 1, 32)
    for n, matrix in enumerate(term_matrices(index_v[...], sign_v[...])):
        terms[n] = matrix
    pl.semaphore_wait(barrier, devices - 1)

    to_core = remote(full.at[other], from_core, core_sem.at[0], core_sem.at[1], z, other)
    to_core.start()

    def send_index(i, carry):
        peer = lax.rem(z + far_first(i, chips), chips)
        for n in range(2):
            mine = idx_send.at[2 * lax.rem(peer, 2) + n, peer // 2]
            remote(mine, idx_recv.at[me], idx_sem.at[0], idx_sem.at[1], peer, n).start()
        return carry

    lax.fori_loop(0, chips - 1, send_index, 0)
    remote(idx_send.at[2 * lax.rem(z, 2) + other, z // 2], idx_recv.at[me], idx_sem.at[0], idx_sem.at[1], z, other).start()
    idx_recv[me] = idx_send[lax.rem(me, 4), z // 2]

    to_core.wait()
    chip_sum[...] = (full[core] + from_core[...]) * scale_in

    times = lax.broadcasted_iota(jnp.int32, weights_v.shape, 0)
    weights = jnp.sum(jnp.where(times == sink_v[...].reshape(1, 1, 1), weights_v[...], 0.0), axis=0)
    weights = jnp.concatenate([weights, jnp.zeros((6, NVEC), F32)], axis=0)
    by_weight = dot(weights, chip_sum[...], PRECISE)
    weighted_rows = by_weight[0:1] * pick_v[0] + by_weight[1:2] * pick_v[1]
    weighted_part = dot(weighted_rows, fold_v[1], PRECISE)
    beside = jnp.concatenate([jnp.zeros((8, 384), F32), weighted_part], axis=1)

    def pack(zz, carry):
        rows = pl.ds(pl.multiple_of(zz * 8, 8), 8)
        rs_send[zz] = (chip_sum[rows] + beside).astype(BF16)
        return carry

    lax.fori_loop(0, chips, pack, 0)

    def send_part(i, carry):
        peer = lax.rem(z + far_first(i, chips), chips)
        remote(rs_send.at[peer], rs_recv.at[z], rs_sem.at[0], rs_sem.at[1], peer, core).start()
        return carry

    lax.fori_loop(0, chips - 1, send_part, 0)
    rs_recv[z] = rs_send[z]

    some = pl.ds(0, devices - 1)
    pltpu.make_async_copy(idx_recv.at[some], idx_recv.at[some], idx_sem.at[1]).wait()

    def reorder(g, carry):
        columns = pl.ds(pl.multiple_of(g * GROUP, GROUP), GROUP)
        wanted = jnp.concatenate([idx_recv[g * 8 + n] for n in range(8)], axis=1) - me * length

        def one_hot(rb, inner):
            rows = pl.ds(pl.multiple_of(rb * 64, 64), 64)
            here = lax.broadcasted_iota(jnp.int32, (64, GROUP), 0) + rb * 64
            perm[rows] = jnp.where(here == wanted, 1.0, 0.0).astype(BF16)
            return inner

        lax.fori_loop(0, length // 64, one_hot, 0)
        for a in range(3):
            eig_p[a, :, columns] = dot(eig_v[a], perm[...]).astype(BF16)
        turned = dot(pieces_v[...], perm[...])
        phase_p[:, columns] = jnp.concatenate([turned[0:4] + turned[4:8] + turned[8:12], jnp.zeros((4, GROUP), F32)], axis=0)
        return carry

    lax.fori_loop(0, length // GROUP, reorder, 0)

    some = pl.ds(0, chips - 1)
    pltpu.make_async_copy(rs_recv.at[some], rs_recv.at[some], rs_sem.at[1]).wait()
    total = jnp.zeros((8, 512), F32)
    total_cos = jnp.zeros((8, 512), F32)
    total_sin = jnp.zeros((8, 512), F32)
    for zz in range(chips):
        part = rs_recv[zz].astype(F32)
        total = total + part
        total_cos = total_cos + phase_v[zz, 0:1, 0:1] * part
        total_sin = total_sin + phase_v[zz, 1:2, 0:1] * part
    masks = pick_v[0]
    blocks = [total * masks[r : r + 1] for r in range(6)]
    blocks.append(total_cos * masks[0:1] + total_sin * masks[1:2])
    blocks.append(total_cos * masks[1:2] - total_sin * masks[0:1])
    block_rows = dot(jnp.concatenate(blocks, axis=0), fold_v[0], PRECISE)
    tails = [pltpu.roll(t[:, 384:512], LANES - 48, 1) for t in (total, total_cos, total_sin)]
    weighted = jnp.concatenate(
        [tails[0][0:6], tails[1][0:1] + tails[2][1:2], tails[1][1:2] - tails[2][0:1]], axis=0
    )
    first = dot(block_rows, terms[0], PRECISE)
    second = dot(weighted, terms[1], PRECISE)
    products = []
    for p in range(NMOM):
        first_re, first_im = first[16 * p : 16 * p + 8], first[16 * p + 8 : 16 * p + 16]
        second_re, second_im = second[2 * p : 2 * p + 1], second[2 * p + 1 : 2 * p + 2]
        products.append(first_re * second_re - first_im * second_im)
        products.append(first_re * second_im + first_im * second_re)
    coeffs = dot_nt(jnp.concatenate(products, axis=0), terms[2], PRECISE)
    piece = jnp.concatenate([coeffs[8 * b : 8 * b + 8, 0:72] for b in range(8)] + [jnp.zeros((8, 64), F32)], axis=1)
    member, quad = lax.rem(z, 4), z // 4
    quads = chips // 4
    gathered[core, member, quad] = piece.astype(BF16)

    def send_far(i, carry):
        peer = lax.rem(quad + far_first(i, quads), quads)
        mine = gathered.at[core, member, quad]
        remote(mine, mine, near_sem.at[0], ag_sem.at[quad], 4 * peer + member, core).start()
        return carry

    lax.fori_loop(0, quads - 1, send_far, 0)

    def spread(came):
        for o in (2, 1, 3):
            remote(came, came, near_sem.at[1], side_sem.at[member], 4 * quad + lax.rem(member + o, 4), core).start()

    spread(gathered.at[core, member, quad])

    def hand_on(i, carry):
        peer = lax.rem(quad + far_first(quads - 2 - i, quads), quads)
        came = gathered.at[core, member, peer]
        pltpu.make_async_copy(came, came, ag_sem.at[peer]).wait()
        spread(came)
        return carry

    lax.fori_loop(0, quads - 1, hand_on, 0)
    for o in range(4):
        whose = lax.rem(member + o, 4)
        theirs = gathered.at[core, whose]
        if o:
            pltpu.make_async_copy(theirs, theirs, side_sem.at[whose]).wait()
        remote(theirs, theirs, both_send, both_sem.at[whose], z, other).start()
    for o in range(4):
        theirs = gathered.at[other, o]
        pltpu.make_async_copy(theirs, theirs, both_sem.at[o]).wait()

    for h in range(2):
        for lb in range(5):
            lanes = slice(lb * LANES, (lb + 1) * LANES)
            tall = jnp.concatenate([gathered[h, zz % 4, zz // 4, :, lanes].astype(F32) for zz in range(chips)], axis=0)
            coeff_t[h, lanes] = tall.T
    for a in range(3):
        def rows_of(q, sign=1.0):
            taken = [
                coeff_t[h, (2 * p + q) * 72 + a * HALF : (2 * p + q) * 72 + (a + 1) * HALF]
                for p in range(NMOM)
                for h in range(2)
            ]
            return (sign * jnp.concatenate(taken, axis=0)).astype(BF16)

        left[a, 0:192, 0:NVEC] = rows_of(0)
        left[a, 0:192, NVEC:] = rows_of(1, -1.0)
        left[a, 192:384, 0:NVEC] = rows_of(1)
        left[a, 192:384, NVEC:] = rows_of(0)

    cos_z, sin_z = phase_v[z, 0:1, 0:1], phase_v[z, 1:2, 0:1]
    groups = length // GROUP
    my_group = me // 8

    def rebuild(i, carry):
        g = lax.rem(my_group + jnp.where(i == groups - 1, 0, far_first(i, groups)), groups)
        columns = pl.ds(pl.multiple_of(g * GROUP, GROUP), GROUP)
        table = phase_p[:, columns]
        cos_x, sin_x, cos_y, sin_y = (table[n : n + 1] for n in range(4))
        for a in range(3):
            both = dot(left[a], eig_p[a, :, columns])
            re = [both[48 * p : 48 * p + 48] for p in range(NMOM)]
            im = [both[192 + 48 * p : 240 + 48 * p] for p in range(NMOM)]
            out_re = re[0] + (cos_x * re[1] - sin_x * im[1]) + (cos_y * re[2] - sin_y * im[2]) + (cos_z * re[3] - sin_z * im[3])
            out_im = im[0] + (cos_x * im[1] + sin_x * re[1]) + (cos_y * im[2] + sin_y * re[2]) + (cos_z * im[3] + sin_z * re[3])
            source[48 * a : 48 * a + 48] = out_re * scale_out
            source[144 + 48 * a : 192 + 48 * a] = out_im * scale_out
        for k in range(2):
            tiles = [source[72 * q : 72 * q + 72, k * LANES : (k + 1) * LANES] for q in range(4)]
            for n, message in enumerate(swap_blocks(tiles, lane_blocks())):
                to_send[g * 8 + 4 * k + n] = message.reshape(9, 8, LANES).astype(BF16)
        for n in range(8):
            peer = g * 8 + n

            @pl.when(peer != me)
            def _():
                remote(to_send.at[peer], arrived.at[me], all_send, all_sem.at[z // 2], peer // 2, n % 2).start()

        return carry

    lax.fori_loop(0, groups, rebuild, 0)
    arrived[me] = to_send[me]

    source_pairs = chips // 2

    def place(group):
        tiles = [arrived[4 * group + d].astype(F32).reshape(72, LANES) for d in range(4)]
        rows = jnp.concatenate(swap_blocks(tiles, lane_blocks()), axis=0)
        columns = pl.ds(pl.multiple_of(group * LANES, LANES), LANES)
        for q in range(2):
            for a in range(3):
                base = q * 144 + a * 48
                result[q, a, :, :, columns] = rows[base : base + 48].reshape(12, 4, LANES).astype(BF16)
        pltpu.make_async_copy(result.at[:, :, :, :, columns], out.at[:, :, :, :, columns], out_sem).start()

    def finish(i, carry):
        group = lax.rem(z // 2 + far_first(i, source_pairs), source_pairs)
        four = arrived.at[pl.ds(4 * group, 4)]
        pltpu.make_async_copy(four, four, all_sem.at[group]).wait()
        place(group)
        return carry

    lax.fori_loop(0, source_pairs - 1, finish, 0)
    three = arrived.at[pl.ds(0, 3)]
    pltpu.make_async_copy(three, three, all_sem.at[z // 2]).wait()
    place(z // 2)

    def drain(ref, sem):
        pltpu.make_async_copy(ref, ref, sem).wait()

    drain(idx_recv.at[pl.ds(0, devices - 1)], idx_sem.at[0])
    drain(rs_send.at[pl.ds(0, chips - 1)], rs_sem.at[0])
    drain(gathered.at[0, 0, pl.ds(0, quads - 1)], near_sem.at[0])
    drain(gathered.at[0, pl.ds(0, 3)], near_sem.at[1])
    drain(gathered.at[0], both_send)
    drain(to_send.at[pl.ds(0, devices - 1)], all_send)
    drain(result, out_sem)


def on_device(propagator, eigvecs, operator_weights, sink_time, term_index, term_sign, solver_order):
    length = propagator.shape[-1]
    chips = lax.axis_size("space_0")
    devices = lax.axis_size(SPACE)
    scale_in = 1.0 / math.sqrt(3.0 * length * devices)
    scale_out = 1.0 / math.sqrt(NMOM * NVEC)
    tables, pieces, chip_phase, pick, fold = fixed_tables(length, chips)
    hbm = pl.BlockSpec(memory_space=pl.ANY)
    arrived = pltpu.VMEM((devices, 9, 8, LANES), BF16)
    result = pl.pallas_call(
        functools.partial(whole_kernel, chips, length, scale_in, scale_out),
        out_shape=jax.ShapeDtypeStruct((2, 3, 12, 4, length), BF16),
        in_specs=[hbm] * 12,
        out_specs=hbm,
        scratch_shapes=[
            pltpu.VMEM((3, 2 * NVEC, length), BF16),
            pltpu.VMEM((2, 3, 12, 4, length), BF16),
            pltpu.VMEM(operator_weights.shape, F32),
            pltpu.VMEM((1, 1), jnp.int32),
            pltpu.VMEM((devices // 4, LANES), jnp.int32),
            pltpu.VMEM((3, NTERM), jnp.int32),
            pltpu.VMEM((1, NTERM), jnp.int32),
            pltpu.VMEM(tables.shape[1:], F32),
            pltpu.VMEM(pieces.shape[1:], BF16),
            pltpu.VMEM(chip_phase.shape, F32),
            pltpu.VMEM(pick.shape, F32),
            pltpu.VMEM(fold.shape, F32),
            pltpu.VMEM((2, 3, NVEC, 144), F32),
            pltpu.VMEM((2, NVEC, 512), F32),
            pltpu.VMEM((NVEC, 512), F32),
            pltpu.VMEM((NVEC, 512), F32),
            pltpu.VMEM((chips, 8, 512), BF16),
            pltpu.VMEM((chips, 8, 512), BF16),
            pltpu.VMEM((4, devices // 4, 1, 32), jnp.int32),
            pltpu.VMEM((devices, 1, 32), jnp.int32),
            pltpu.VMEM((3, LANES, 384), F32),
            pltpu.VMEM((length, GROUP), BF16),
            pltpu.VMEM((3, 2 * NVEC, length), BF16),
            pltpu.VMEM((8, length), F32),
            pltpu.VMEM((2, 4, chips // 4, 8, 640), BF16),
            pltpu.VMEM((2, 640, NVEC), F32),
            pltpu.VMEM((3, 384, 2 * NVEC), BF16),
            pltpu.VMEM((288, GROUP), F32),
            arrived,
            arrived,
            pltpu.VMEM((2, 3, 12, 4, length), BF16),
            pltpu.SemaphoreType.DMA((12,)),
            pltpu.SemaphoreType.DMA((10,)),
            pltpu.SemaphoreType.DMA((2,)),
            pltpu.SemaphoreType.DMA((2,)),
            pltpu.SemaphoreType.DMA((2,)),
            pltpu.SemaphoreType.DMA((2,)),
            pltpu.SemaphoreType.DMA((chips // 4,)),
            pltpu.SemaphoreType.DMA((4,)),
            pltpu.SemaphoreType.DMA,
            pltpu.SemaphoreType.DMA((4,)),
            pltpu.SemaphoreType.DMA,
            pltpu.SemaphoreType.DMA((chips // 2,)),
            pltpu.SemaphoreType.DMA,
        ],
        compiler_params=pltpu.CompilerParams(collective_id=0, has_side_effects=True, vmem_limit_bytes=56 * 2**20),
    )(
        eigvecs, jnp.swapaxes(propagator, 2, 3), operator_weights, sink_time.reshape(1, 1), solver_order.reshape(devices // 4, LANES),
        term_index.T, term_sign.reshape(1, -1), jnp.asarray(tables), jnp.asarray(pieces), jnp.asarray(chip_phase),
        jnp.asarray(pick), jnp.asarray(fold),
    )
    return jnp.swapaxes(result, 2, 3)


def solution(mesh):
    finer = Mesh(mesh.devices.reshape(mesh.shape["grp"], -1, 2), ("grp", "space_0", "space_1"))
    in_specs = (
        P("grp", None, None, None, SPACE),
        P("grp", None, None, SPACE),
        P("grp", None, None),
        P("grp"),
        P(),
        P(),
        P(SPACE),
    )
    out_specs = P("grp", None, None, None, SPACE)
    return jax.shard_map(on_device, mesh=finer, in_specs=in_specs, out_specs=out_specs, check_vma=False)
```
